32 devices in a mesh: section: 4 (over y, core), dp: 8 (over z, x).
Axes of the slice: x: 2, y: 2, z: 4, core: 2. Of those that a mesh axis runs over, the one named last changes fastest.
Arguments:
- tokens: bfloat16 [64, 6144], P('dp', 'section'), may hold values from -6 to 6
- expert_ids: int32 [64, 2], P('dp'), may hold values from 0 to 7, all different within a row; in each aligned block of 8 rows (0 to 7, 8 to 15, ...) at most 4 rows name the same one
- router: bfloat16 [6144, 8], replicated, may hold values from -0.078125 to 0.078125
- w_up: bfloat16 [8, 6144, 16384], P('dp', None, 'section'), may hold values from -0.078125 to 0.078125
- w_down: bfloat16 [8, 16384, 6144], P('dp', 'section'), may hold values from -0.0625 to 0.0625
- attn_queries: bfloat16 [8, 128, 6144], P('dp', None, 'section'), may hold values from -140 to 140
- attn_keys: bfloat16 [8, 128, 6144], P('dp', None, 'section'), may hold values from -8 to 8
- attn_values: bfloat16 [8, 128, 6144], P('dp', None, 'section'), may hold values from -6 to 6
Outputs:
- mixed: bfloat16 [64, 6144], P('dp', 'section')
- attended: bfloat16 [8, 128, 6144], P('dp', None, 'section')
The draws below stay inside these ranges and needn't reach their ends.
Inputs may be any that keep to these rules, and one draw needn't show every extreme that they name: `expert_ids`: each row names two different experts; among the 8 rows of one dp index (aligned blocks) no expert is named more than 4 times.
All inputs are finite; a program needn't handle non-finite values.
Results may differ from the reference program's by a relative error of at most 0.005.
Values may be sent and summed in bfloat16 or wider, within the bound.
A program may use at most 192 MiB of HBM per device.

```python
import math
import jax
import jax.numpy as jnp
import numpy as np
from jax import lax

D = 6144
FF = 16384
EXPERTS = 8
ATT_HEADS = 48
HEAD_DIM = 128
CAP = 4
TOK_DP = 8
SEQ = 128
RSPLIT = 1
TOKENS = 64
N_DP = 8


def attention_pair(key):
    base = jax.random.fold_in(key, 7)
    key_query, key_keys = jax.random.split(base, 2)
    shape = (N_DP, SEQ, ATT_HEADS * HEAD_DIM)
    key_array = jnp.clip(jax.random.normal(key_keys, shape, jnp.float32), -6.0, 6.0)
    query_array = jnp.clip(jax.random.normal(key_query, shape, jnp.float32), -6.0, 6.0)
    return (query_array, key_array)


def draw_attn_queries(key, part):
    query_array, key_array = attention_pair(key)
    return query_array.astype(jnp.bfloat16)


def draw_attn_keys(key, part):
    query_array, key_array = attention_pair(key)
    return key_array.astype(jnp.bfloat16)


def raised(result, rng, source, target, shards_of, factor):
    def block_of(position):
        return (jnp.arange(result.shape[position]) // (result.shape[position] // shards_of)).reshape((-1,) + (1,) * (result.ndim - 1 - position))

    near = jax.random.permutation(rng, shards_of)[block_of(target)]
    second = (block_of(target) + shards_of // 2) % shards_of
    return jnp.where((block_of(source) == near) | (block_of(source) == second), factor * result, result)


def levels(stream_key, extent, cuts, smallest, high):
    loudness, own = 1.0, jax.random.fold_in(stream_key, 6)
    for dim, blocks in cuts:
        draws = jnp.exp(jax.random.uniform(jax.random.fold_in(own, dim), (blocks,), jnp.float32, smallest / len(cuts), high / len(cuts)))
        loudness = loudness * jnp.repeat(draws, extent[dim] // blocks).reshape([-1 if axis == dim else 1 for axis in range(len(extent))])
    return loudness


def shared_out(key, own, number, rows, amount, top, limit, skew):
    sequence = jax.random.permutation(key, amount)
    packed, usual = shares(amount, rows * top, limit, skew, True), shares(amount, rows * top, limit, skew, False)
    places = jnp.arange(amount)

    def named(sizes, rotation):
        used = int((sizes > 0).sum())
        fixed = max(1, used // 4)
        passed = fixed + (places - fixed + rotation * (used - fixed)) % max(1, amount - fixed)
        return jnp.zeros((amount,), jnp.int32).at[sequence[jnp.where(places < fixed, places, passed)]].set(jnp.asarray(sizes, jnp.int32))

    sizes = jnp.where(number % 4 == 0, named(packed, number // 4), named(usual, number - number // 4 - 1))
    mixed = jax.random.permutation(jax.random.fold_in(own, 3), amount)
    giver, receiver = mixed[0:amount // 2 * 2:2], mixed[1:amount // 2 * 2:2]
    margin = jnp.minimum(sizes[giver] - 1, limit - sizes[receiver]) // 2
    margin = jnp.where((giver == sequence[0]) | (receiver == sequence[0]) | (sizes[receiver] == 0), 0, jnp.maximum(margin, 0))
    passed = jax.random.randint(jax.random.fold_in(own, 4), (amount // 2,), 0, 1 << 20) % (margin + 1)
    sizes = sizes.at[giver].add(-passed).at[receiver].add(passed)
    labels = jnp.searchsorted(jnp.cumsum(sizes), jnp.arange(rows * top), side="right").astype(jnp.int32)
    grid = labels.reshape(top, rows).T
    grid = grid[jax.random.permutation(jax.random.fold_in(own, 1), rows)]
    rotation = jax.random.randint(jax.random.fold_in(own, 2), (rows, 1), 0, top)
    return jnp.take_along_axis(grid, (jnp.arange(top)[None, :] + rotation) % top, axis=1)


def shares(count, total, limit, skew, full):
    loads = [(1 << 20) // math.isqrt(rank ** skew) + 1 for rank in range(1, count + 1)]
    largest = limit if full else min(limit, max(-(-total // count), total * loads[0] // sum(loads)))
    least = 1 if total - largest >= count - 1 else 0
    given, surplus = [largest] + [least] * (count - 1), total - largest - least * (count - 1)
    while surplus > 0:
        candidates = [i for i in range(1, count) if given[i] < largest] or [i for i in range(1, count) if given[i] < limit]
        mass, left = sum([loads[i] for i in candidates]), surplus
        for i in candidates:
            extra = min(limit - given[i], max(1, left * loads[i] // mass), surplus)
            given[i] = given[i] + extra
            surplus = surplus - extra
    return np.array(given)


def gaussian(stream_key, extent, deviation, most, cuts=(), held_as=jnp.bfloat16):
    entries = deviation * jax.random.normal(stream_key, extent, jnp.float32)
    if cuts:
        entries = entries * levels(stream_key, extent, cuts, -0.22, 0.18)
    return jnp.clip(entries, -most, most).astype(held_as)


def heavy_noise(stream_key, shape, spread, reach, pieces, heavy, held_as=jnp.bfloat16):
    result = spread * jax.random.normal(stream_key, shape, jnp.float32)
    if pieces:
        result = result * levels(stream_key, shape, pieces, -0.22, 0.18)
    return jnp.clip(raised(result, jax.random.fold_in(stream_key, 3), *heavy), -reach, reach).astype(held_as)


def setup_inputs(seed: int = 0) -> dict:
    key_of = jax.random.split(jax.random.key(seed), 9)
    tokens = gaussian(key_of[0], (TOKENS, D), 1.0, 6.0, ((0, 8), (1, 4)))
    expert_ids_keys = jax.random.split(jax.random.fold_in(key_of[1], 1), TOKENS // TOK_DP)
    expert_ids_turns = jax.random.permutation(jax.random.fold_in(key_of[1], 3), TOKENS // TOK_DP)
    expert_ids = jax.vmap(lambda own, number: shared_out(jax.random.fold_in(key_of[1], 2), own, number, TOK_DP, EXPERTS, 2, CAP, 2))(expert_ids_keys, expert_ids_turns).reshape((TOKENS, 2))
    router = gaussian(key_of[2], (D, EXPERTS), D ** -0.5, 0.078125)
    w_up = gaussian(key_of[3], (N_DP, D, FF // RSPLIT), D ** -0.5, 0.078125, ((0, 8), (2, 4)))
    w_down = heavy_noise(key_of[4], (N_DP, FF // RSPLIT, D), FF ** -0.5, 0.0625, ((0, 8), (1, 4)), (1, 2, 4, 2.0))
    attn_queries = draw_attn_queries(jax.random.fold_in(key_of[8], 71), 0)
    attn_keys = draw_attn_keys(jax.random.fold_in(key_of[8], 71), 0)
    attn_values = gaussian(key_of[7], (N_DP, SEQ, ATT_HEADS * HEAD_DIM), 1.0, 6.0, ((0, 8), (2, 4)))
    return dict(tokens=tokens, expert_ids=expert_ids, router=router, w_up=w_up, w_down=w_down, attn_queries=attn_queries, attn_keys=attn_keys, attn_values=attn_values)


def pair_weights(tokens, router, expert_ids):
    logits = jnp.dot(tokens, router, preferred_element_type=jnp.float32)
    experts = router.shape[1]
    onehot = (expert_ids[:, :, None] == jnp.arange(experts, dtype=jnp.int32)[None, None, :]).astype(jnp.float32)
    chosen = lax.optimization_barrier(jnp.sum(logits[:, None, :] * onehot, axis=2))
    first_prob = jax.nn.sigmoid(chosen[:, 0] - chosen[:, 1])
    return jnp.stack([first_prob, 1.0 - first_prob], axis=1)

def route_slots(expert_ids, block_count, per_block, experts):
    pair_ids = expert_ids.reshape(block_count, per_block * 2)
    onehot = (pair_ids[:, :, None] == jnp.arange(experts, dtype=jnp.int32)[None, None, :]).astype(jnp.int32)
    before = jnp.cumsum(onehot, axis=1) - onehot
    slot_rank = lax.optimization_barrier(jnp.sum(before * onehot, axis=2))
    return slot_rank.reshape(block_count * per_block, 2)

def attend_head(operands):
    head_queries, head_keys, head_values = operands
    length = head_queries.shape[0]
    scores = jnp.dot(head_queries, head_keys.T, preferred_element_type=jnp.float32) * (1.0 / math.sqrt(head_queries.shape[1]))
    positions = jnp.arange(length, dtype=jnp.int32)
    causal = positions[None, :] <= positions[:, None]
    scores = jnp.where(causal, scores, -jnp.inf)
    row_max = lax.optimization_barrier(jnp.max(scores, axis=1, keepdims=True))
    exp_scores = jnp.exp(scores - row_max)
    row_total = lax.optimization_barrier(jnp.sum(exp_scores, axis=1, keepdims=True))
    probs = (exp_scores / row_total).astype(jnp.bfloat16)
    return jnp.dot(probs, head_values, preferred_element_type=jnp.float32).astype(jnp.bfloat16)

def attention(attn_queries, attn_keys, attn_values):
    batch, length, width = attn_queries.shape
    heads = width // HEAD_DIM

    def split_heads(array):
        return jnp.transpose(array.reshape(batch, length, heads, HEAD_DIM), (0, 2, 1, 3)).reshape(batch * heads, length, HEAD_DIM)
    outputs = lax.map(attend_head, (split_heads(attn_queries), split_heads(attn_keys), split_heads(attn_values)))
    return jnp.transpose(outputs.reshape(batch, heads, length, HEAD_DIM), (0, 2, 1, 3)).reshape(batch, length, width)

def reference(tokens, expert_ids, router, w_up, w_down, attn_queries, attn_keys, attn_values):
    token_count, model_width = tokens.shape
    experts = router.shape[1]
    block_count = w_up.shape[0]
    split_count = block_count // experts
    per_block = token_count // block_count
    slot_count = block_count * CAP
    pair_prob = pair_weights(tokens, router, expert_ids)
    slot_rank = route_slots(expert_ids, block_count, per_block, experts)
    block_of = (jnp.arange(token_count, dtype=jnp.int32) // per_block)[:, None]
    slot_of = block_of * CAP + slot_rank
    slot_range = jnp.arange(slot_count, dtype=jnp.int32)
    token_rows = tokens.astype(jnp.float32)

    def one_expert(carried, expert):
        chosen_here = expert_ids == expert
        matched = (slot_of[:, :, None] == slot_range[None, None, :]) & chosen_here[:, :, None]
        selector = jnp.any(matched, axis=1).astype(jnp.float32)
        weighting = lax.optimization_barrier(jnp.sum(matched.astype(jnp.float32) * pair_prob[:, :, None], axis=1))
        rows = jnp.dot(selector.T, token_rows, precision=lax.Precision.HIGHEST).astype(jnp.bfloat16)
        first = (expert * split_count).astype(jnp.int32)
        up_part = lax.dynamic_slice_in_dim(w_up, first, split_count, 0)
        up_full = jnp.transpose(up_part, (1, 0, 2)).reshape(model_width, -1)
        down_full = lax.dynamic_slice_in_dim(w_down, first, split_count, 0).reshape(-1, model_width)
        activated = jax.nn.silu(jnp.dot(rows, up_full, preferred_element_type=jnp.float32)).astype(jnp.bfloat16)
        expert_out = jnp.dot(activated, down_full, preferred_element_type=jnp.float32)
        return (carried + jnp.dot(weighting, expert_out, precision=lax.Precision.HIGHEST), None)
    summed, _ = lax.scan(one_expert, jnp.zeros((token_count, model_width), jnp.float32), jnp.arange(experts, dtype=jnp.int32))
    attended = attention(attn_queries, attn_keys, attn_values)
    return (summed.astype(jnp.bfloat16), attended)
```

```python
import functools
import math

import jax
import jax.numpy as jnp
from jax import lax
from jax.experimental import pallas as pl
from jax.experimental.pallas import tpu as pltpu
from jax.sharding import PartitionSpec as P

HEAD_DIM = 128
MESH = pl.DeviceIdType.MESH


def aligned(index, size):
    return pl.ds(pl.multiple_of(index * size, size), size)


def kernel(
    dims,
    tokens_hbm,
    ids_hbm,
    router_hbm,
    up_hbm,
    down_hbm,
    q_hbm,
    k_hbm,
    v_hbm,
    mixed_hbm,
    attended_hbm,
    ring,
    x_all,
    x_rows,
    hidden,
    stage,
    received,
    router,
    ids,
    logits,
    q,
    k,
    v,
    attended,
    mixed,
    small_sem,
    up_sem,
    down_sem,
    send_sem,
    x_sem,
    back_sem,
    part_sem,
    own_sem,
    out_sem,
):
    n_sec, n_dp, rows, cols, experts = dims
    per_block, width = tokens_hbm.shape
    model, ff = up_hbm.shape[1:]
    devices = n_sec * n_dp
    up_blocks, up_units = ff // cols, model // rows
    down_blocks, down_units = model // cols, ff // rows
    sec_blocks = width // cols
    s, g = lax.axis_index("section"), lax.axis_index("dp")
    me = s * n_dp + g

    copies = [
        pltpu.make_async_copy(tokens_hbm, x_all.at[me], small_sem.at[0]),
        pltpu.make_async_copy(q_hbm.at[0], q, small_sem.at[1]),
        pltpu.make_async_copy(k_hbm.at[0], k, small_sem.at[2]),
        pltpu.make_async_copy(v_hbm.at[0], v, small_sem.at[3]),
        pltpu.make_async_copy(router_hbm, router, small_sem.at[4]),
        pltpu.make_async_copy(ids_hbm, ids, small_sem.at[5]),
    ]
    for copy in copies:
        copy.start()

    def up_copy(n):
        return pltpu.make_async_copy(
            up_hbm.at[0, :, aligned(n, cols)], ring.at[aligned(n, model)], up_sem.at[n]
        )

    @pl.loop(0, up_blocks)
    def _(n):
        up_copy(n).start()

    barrier = pltpu.get_barrier_semaphore()

    def place(index):
        return {"section": index // n_dp, "dp": index % n_dp}

    @pl.loop(1, devices)
    def _(offset):
        peer = (me + offset) % devices
        pl.semaphore_signal(barrier, inc=1, device_id=place(peer), device_id_type=MESH)

    copies[0].wait()
    pl.semaphore_wait(barrier, devices - 1)

    @pl.loop(1, devices)
    def _(offset):
        peer = (me + offset) % devices
        pltpu.make_async_remote_copy(
            src_ref=x_all.at[me],
            dst_ref=x_all.at[me],
            send_sem=send_sem,
            recv_sem=x_sem,
            device_id=place(peer),
            device_id_type=MESH,
        ).start()

    for copy in copies[1:4]:
        copy.wait()
    length = q.shape[0]
    heads = width // HEAD_DIM
    group = math.gcd(heads, 4)
    causal = lax.broadcasted_iota(jnp.int32, (length, length), 1) <= lax.broadcasted_iota(
        jnp.int32, (length, length), 0
    )

    @pl.loop(0, heads // group)
    def _(step):
        for lane in range(group):
            at = aligned(step * group + lane, HEAD_DIM)
            scores = lax.dot_general(
                q[:, at], k[:, at], (((1,), (1,)), ((), ())), preferred_element_type=jnp.float32
            ) * (1.0 / math.sqrt(HEAD_DIM))
            scores = jnp.where(causal, scores, -jnp.inf)
            exps = jnp.exp(scores - jnp.max(scores, axis=1, keepdims=True))
            probs = (exps / jnp.sum(exps, axis=1, keepdims=True)).astype(jnp.bfloat16)
            attended[:, at] = jnp.dot(
                probs, v[:, at], preferred_element_type=jnp.float32
            ).astype(jnp.bfloat16)

    attended_copy = pltpu.make_async_copy(attended, attended_hbm.at[0], out_sem.at[0])
    attended_copy.start()

    others = x_all.at[pl.ds(0, devices - 1)]
    pltpu.make_async_copy(others, others, x_sem).wait()
    for part in range(n_sec):
        at = pl.ds(part * width, width)
        for pair in range(n_dp // 2):
            first = x_all[part * n_dp + 2 * pair].astype(jnp.float32)
            second = x_all[part * n_dp + 2 * pair + 1].astype(jnp.float32)
            x_rows[pl.ds(2 * pair * per_block, 2 * per_block), at] = jnp.concatenate(
                [first, second], axis=0
            ).astype(jnp.bfloat16)

    def down_place(block):
        return (s + 1 + block // sec_blocks) % n_sec, block % sec_blocks

    def down_copy(unit):
        block, part = unit // down_units, unit % down_units
        sec, col = down_place(block)
        return pltpu.make_async_copy(
            down_hbm.at[0, aligned(part, rows), aligned(sec * sec_blocks + col, cols)],
            ring.at[aligned(unit, rows)],
            down_sem.at[block],
        )

    @pl.loop(0, up_blocks)
    def _(n):
        up_copy(n).wait()
        value = jnp.dot(
            x_rows[...], ring[aligned(n, model), :], preferred_element_type=jnp.float32
        )
        hidden[:, aligned(n, cols)] = (value / (1.0 + jnp.exp(-value))).astype(jnp.bfloat16)
        for unit in range(up_units):
            down_copy(n * up_units + unit).start()

    copies[4].wait()
    copies[5].wait()
    logits[...] = lax.dot_general(
        x_rows[...], router[...], (((1,), (1,)), ((), ())), preferred_element_type=jnp.float32
    )
    own = logits[aligned(g, per_block), :]
    lanes = lax.broadcasted_iota(jnp.int32, (per_block, experts), 1)
    diagonal = lax.broadcasted_iota(jnp.int32, (per_block, per_block), 0) == lax.broadcasted_iota(
        jnp.int32, (per_block, per_block), 1
    )

    def column(which):
        row = jnp.broadcast_to(ids[which : which + 1, :].astype(jnp.float32), diagonal.shape)
        return jnp.sum(jnp.where(diagonal, row, 0.0), axis=1, keepdims=True).astype(jnp.int32)

    is_first, is_second = column(0) == lanes, column(1) == lanes
    gap = jnp.sum(jnp.where(is_first, own, 0.0), axis=1, keepdims=True) - jnp.sum(
        jnp.where(is_second, own, 0.0), axis=1, keepdims=True
    )
    first_prob = 1.0 / (1.0 + jnp.exp(-gap))
    coefficient = jnp.where(is_first, first_prob, 0.0) + jnp.where(
        is_second, 1.0 - first_prob, 0.0
    )

    def down_block(block):
        taken = ring.at[aligned(block, ff)]
        pltpu.make_async_copy(taken, taken, down_sem.at[block]).wait()
        partial = jnp.dot(hidden[...], taken[...], preferred_element_type=jnp.float32)
        for b in range(n_dp):
            stage[block, b] = partial[b * per_block : (b + 1) * per_block].astype(jnp.bfloat16)

    def send_back(block, first):
        sec, col = down_place(block)

        @pl.loop(first, n_dp)
        def _(offset):
            b = (g + offset) % n_dp
            pltpu.make_async_remote_copy(
                src_ref=stage.at[block, b],
                dst_ref=received.at[me, :, aligned(col, cols)],
                send_sem=part_sem,
                recv_sem=back_sem,
                device_id={"section": sec, "dp": b},
                device_id_type=MESH,
            ).start()

    away = (n_sec - 1) * sec_blocks

    @pl.loop(0, away)
    def _(block):
        down_block(block)
        send_back(block, 0)

    @pl.loop(away, down_blocks)
    def _(block):
        down_block(block)
        send_back(block, 1)
        pltpu.make_async_copy(
            stage.at[block, g],
            received.at[me, :, aligned(block - away, cols)],
            own_sem,
        ).start()

    own_row = received.at[me]
    pltpu.make_async_copy(own_row, own_row, own_sem).wait()
    rest = received.at[pl.ds(0, devices - 1)]
    pltpu.make_async_copy(rest, rest, back_sem).wait()

    shares = [
        jnp.broadcast_to(coefficient[:, e : e + 1], (per_block, width)) for e in range(experts)
    ]
    per_expert = n_dp // experts

    def add(part, total):
        for b in range(n_dp):
            total += shares[b // per_expert] * received[part * n_dp + b].astype(jnp.float32)
        return total

    total = lax.fori_loop(0, n_sec, add, jnp.zeros((per_block, width), jnp.float32))
    mixed[...] = total.astype(jnp.bfloat16)
    mixed_copy = pltpu.make_async_copy(mixed, mixed_hbm, out_sem.at[1])
    mixed_copy.start()

    pltpu.make_async_copy(others, others, send_sem).wait()
    pltpu.make_async_copy(rest, rest, part_sem).wait()
    attended_copy.wait()
    mixed_copy.wait()


def per_device(tokens, expert_ids, router, w_up, w_down, attn_queries, attn_keys, attn_values):
    n_sec, n_dp = lax.axis_size("section"), lax.axis_size("dp")
    per_block, width = tokens.shape
    model, experts = router.shape
    ff = w_up.shape[2]
    length = attn_queries.shape[1]
    devices = n_sec * n_dp
    rows, cols = math.gcd(model, ff), math.gcd(ff, width)
    down_blocks = model // cols
    bf16, f32 = jnp.bfloat16, jnp.float32
    any_spec = pl.BlockSpec(memory_space=pl.ANY)
    return pl.pallas_call(
        functools.partial(kernel, (n_sec, n_dp, rows, cols, experts)),
        out_shape=(
            jax.ShapeDtypeStruct(tokens.shape, bf16),
            jax.ShapeDtypeStruct(attn_queries.shape, bf16),
        ),
        in_specs=[any_spec] * 8,
        out_specs=(any_spec, any_spec),
        scratch_shapes=[
            pltpu.VMEM((model * ff // cols, cols), bf16),
            pltpu.VMEM((devices, per_block, width), bf16),
            pltpu.VMEM((n_dp * per_block, model), bf16),
            pltpu.VMEM((n_dp * per_block, ff), bf16),
            pltpu.VMEM((down_blocks, n_dp, per_block, cols), bf16),
            pltpu.VMEM((devices, per_block, width), bf16),
            pltpu.VMEM((experts, model), bf16),
            pltpu.VMEM((2, per_block), jnp.int32),
            pltpu.VMEM((n_dp * per_block, experts), f32),
            pltpu.VMEM((length, width), bf16),
            pltpu.VMEM((length, width), bf16),
            pltpu.VMEM((length, width), bf16),
            pltpu.VMEM((length, width), bf16),
            pltpu.VMEM((per_block, width), bf16),
            pltpu.SemaphoreType.DMA((6,)),
            pltpu.SemaphoreType.DMA((ff // cols,)),
            pltpu.SemaphoreType.DMA((down_blocks,)),
            pltpu.SemaphoreType.DMA,
            pltpu.SemaphoreType.DMA,
            pltpu.SemaphoreType.DMA,
            pltpu.SemaphoreType.DMA,
            pltpu.SemaphoreType.DMA,
            pltpu.SemaphoreType.DMA((2,)),
        ],
        compiler_params=pltpu.CompilerParams(
            collective_id=0, has_side_effects=True, vmem_limit_bytes=67043328
        ),
    )(tokens, expert_ids.T, router.T, w_up, w_down, attn_queries, attn_keys, attn_values)


def solution(mesh):
    placed = (
        P("dp", "section"),
        P("dp", None),
        P(),
        P("dp", None, "section"),
        P("dp", "section", None),
        P("dp", None, "section"),
        P("dp", None, "section"),
        P("dp", None, "section"),
    )
    return jax.shard_map(
        per_device,
        mesh=mesh,
        in_specs=placed,
        out_specs=(P("dp", "section"), P("dp", None, "section")),
        check_vma=False,
    )
```

```python
import functools
import math

import jax
import jax.numpy as jnp
from jax import lax
from jax.experimental import pallas as pl
from jax.experimental.pallas import tpu as pltpu
from jax.sharding import PartitionSpec as P

HEAD_DIM = 128
MESH = pl.DeviceIdType.MESH


def aligned(index, size):
    return pl.ds(pl.multiple_of(index * size, size), size)


def kernel(
    dims,
    tokens_hbm,
    ids_hbm,
    router_hbm,
    up_hbm,
    down_hbm,
    q_hbm,
    k_hbm,
    v_hbm,
    mixed_hbm,
    attended_hbm,
    ring,
    x_all,
    x_rows,
    hidden,
    stage,
    terms,
    returning,
    received,
    router,
    ids,
    logits,
    q,
    k,
    v,
    attended,
    mixed,
    small_sem,
    up_sem,
    down_sem,
    send_sem,
    line_sem,
    plane_sem,
    x_sem,
    term_sem,
    back_sem,
    part_sem,
    own_sem,
    out_sem,
):
    n_sec, n_dp, rows, cols, experts = dims
    per_block, width = tokens_hbm.shape
    model, ff = up_hbm.shape[1:]
    devices = n_sec * n_dp
    up_blocks, up_units = ff // cols, model // rows
    down_blocks, down_units = model // cols, ff // rows
    sec_blocks = width // cols
    s, g = lax.axis_index("section"), lax.axis_index("dp")
    me = s * n_dp + g
    half, lines = n_sec // 2, n_dp // 2
    y, core, line, x = s // 2, s % 2, g // 2, g % 2

    def slot(y_at, core_at, dp):
        return (core_at * half + y_at) * n_dp + dp

    mine = slot(y, core, g)

    copies = [
        pltpu.make_async_copy(tokens_hbm, x_all.at[mine], small_sem.at[0]),
        pltpu.make_async_copy(q_hbm.at[0], q, small_sem.at[1]),
        pltpu.make_async_copy(k_hbm.at[0], k, small_sem.at[2]),
        pltpu.make_async_copy(v_hbm.at[0], v, small_sem.at[3]),
        pltpu.make_async_copy(router_hbm, router, small_sem.at[4]),
        pltpu.make_async_copy(ids_hbm, ids, small_sem.at[5]),
    ]
    for copy in copies:
        copy.start()

    def up_copy(n):
        return pltpu.make_async_copy(
            up_hbm.at[0, :, aligned(n, cols)], ring.at[aligned(n, model)], up_sem.at[n]
        )

    @pl.loop(0, up_blocks)
    def _(n):
        up_copy(n).start()

    barrier = pltpu.get_barrier_semaphore()

    def place(index):
        return {"section": index // n_dp, "dp": index % n_dp}

    @pl.loop(1, devices)
    def _(offset):
        peer = (me + offset) % devices
        pl.semaphore_signal(barrier, inc=1, device_id=place(peer), device_id_type=MESH)

    for copy in copies[1:4]:
        copy.wait()
    length = q.shape[0]
    heads = width // HEAD_DIM
    group = math.gcd(heads, 4)
    causal = lax.broadcasted_iota(jnp.int32, (length, length), 1) <= lax.broadcasted_iota(
        jnp.int32, (length, length), 0
    )

    def attend(third):
        steps = heads // group
        pl.loop(steps * third // 3, steps * (third + 1) // 3)(attend_heads)

    def attend_heads(step):
        for lane in range(group):
            at = aligned(step * group + lane, HEAD_DIM)
            scores = lax.dot_general(
                q[:, at], k[:, at], (((1,), (1,)), ((), ())), preferred_element_type=jnp.float32
            ) * (1.0 / math.sqrt(HEAD_DIM))
            scores = jnp.where(causal, scores, -jnp.inf)
            exps = jnp.exp(scores - jnp.max(scores, axis=1, keepdims=True))
            probs = (exps / jnp.sum(exps, axis=1, keepdims=True)).astype(jnp.bfloat16)
            attended[:, at] = jnp.dot(
                probs, v[:, at], preferred_element_type=jnp.float32
            ).astype(jnp.bfloat16)

    attend(0)
    copies[0].wait()
    pl.semaphore_wait(barrier, devices - 1)

    def send_tokens(block, sem, place):
        pltpu.make_async_remote_copy(
            src_ref=x_all.at[block],
            dst_ref=x_all.at[block],
            send_sem=send_sem,
            recv_sem=sem,
            device_id=place,
            device_id_type=MESH,
        ).start()

    @pl.loop(1, lines)
    def _(offset):
        to = (line + offset) % lines
        send_tokens(mine, line_sem.at[offset], {"section": s, "dp": to * 2 + x})

    def spread(from_line):
        block = slot(y, core, from_line * 2 + x)

        @pl.loop(1, 2 * half)
        def _(offset):
            to_y, to_x = (y + offset // 2) % half, (x + offset) % 2
            send_tokens(
                block, plane_sem, {"section": to_y * 2 + core, "dp": line * 2 + to_x}
            )

    spread(line)
    attend(1)

    @pl.loop(1, lines)
    def _(offset):
        from_line = (line + lines - offset) % lines
        block = x_all.at[slot(y, core, from_line * 2 + x)]
        pltpu.make_async_copy(block, block, line_sem.at[offset]).wait()
        spread(from_line)

    n_half = half * n_dp
    plane = x_all.at[pl.ds(0, n_half - lines)]
    pltpu.make_async_copy(plane, plane, plane_sem).wait()
    send_tokens(pl.ds(core * n_half, n_half), x_sem, {"section": y * 2 + 1 - core, "dp": g})

    attend(2)
    attended_copy = pltpu.make_async_copy(attended, attended_hbm.at[0], out_sem.at[0])
    attended_copy.start()

    others = x_all.at[pl.ds(0, devices - 1)]
    arrived = x_all.at[pl.ds(0, n_half)]
    pltpu.make_async_copy(arrived, arrived, x_sem).wait()
    for part in range(n_sec):
        at = pl.ds((part % half * 2 + part // half) * width, width)
        for pair in range(n_dp // 2):
            first = x_all[part * n_dp + 2 * pair].astype(jnp.float32)
            second = x_all[part * n_dp + 2 * pair + 1].astype(jnp.float32)
            x_rows[pl.ds(2 * pair * per_block, 2 * per_block), at] = jnp.concatenate(
                [first, second], axis=0
            ).astype(jnp.bfloat16)

    def down_place(block):
        turn = block // sec_blocks
        to_y, to_core = (y + 1 + turn // 2) % half, (core + 1 + turn) % 2
        return to_y * 2 + to_core, block % sec_blocks

    def down_copy(unit):
        block, part = unit // down_units, unit % down_units
        sec, col = down_place(block)
        return pltpu.make_async_copy(
            down_hbm.at[0, aligned(part, rows), aligned(sec * sec_blocks + col, cols)],
            ring.at[aligned(unit, rows)],
            down_sem.at[block],
        )

    @pl.loop(0, up_blocks)
    def _(n):
        up_copy(n).wait()
        value = jnp.dot(
            x_rows[...], ring[aligned(n, model), :], preferred_element_type=jnp.float32
        )
        hidden[:, aligned(n, cols)] = (value / (1.0 + jnp.exp(-value))).astype(jnp.bfloat16)
        for unit in range(up_units):
            down_copy(n * up_units + unit).start()

    copies[4].wait()
    copies[5].wait()
    logits[...] = lax.dot_general(
        x_rows[...], router[...], (((1,), (1,)), ((), ())), preferred_element_type=jnp.float32
    )
    own = logits[aligned(g, per_block), :]
    lanes = lax.broadcasted_iota(jnp.int32, (per_block, experts), 1)
    diagonal = lax.broadcasted_iota(jnp.int32, (per_block, per_block), 0) == lax.broadcasted_iota(
        jnp.int32, (per_block, per_block), 1
    )

    def column(which):
        row = jnp.broadcast_to(ids[which : which + 1, :].astype(jnp.float32), diagonal.shape)
        return jnp.sum(jnp.where(diagonal, row, 0.0), axis=1, keepdims=True).astype(jnp.int32)

    is_first, is_second = column(0) == lanes, column(1) == lanes
    gap = jnp.sum(jnp.where(is_first, own, 0.0), axis=1, keepdims=True) - jnp.sum(
        jnp.where(is_second, own, 0.0), axis=1, keepdims=True
    )
    first_prob = 1.0 / (1.0 + jnp.exp(-gap))
    coefficient = jnp.where(is_first, first_prob, 0.0) + jnp.where(
        is_second, 1.0 - first_prob, 0.0
    )

    def down_block(block):
        taken = ring.at[aligned(block, ff)]
        pltpu.make_async_copy(taken, taken, down_sem.at[block]).wait()
        return jnp.dot(hidden[...], taken[...], preferred_element_type=jnp.float32)

    away = (n_sec - 1) * sec_blocks

    @pl.loop(0, away)
    def _(block):
        stage[block] = down_block(block).astype(jnp.bfloat16)
        sec, col = down_place(block)
        pltpu.make_async_remote_copy(
            src_ref=stage.at[block],
            dst_ref=terms.at[block // sec_blocks, :, aligned(col, cols)],
            send_sem=term_sem.at[0],
            recv_sem=term_sem.at[1],
            device_id={"section": sec, "dp": g},
            device_id_type=MESH,
        ).start()

    pltpu.make_async_copy(terms, terms, term_sem.at[1]).wait()

    @pl.loop(away, down_blocks)
    def _(block):
        at = aligned(block - away, cols)
        summed = down_block(block)
        for term in range(n_sec - 1):
            summed += terms[term, :, at].astype(jnp.float32)
        for b in range(n_dp):
            returning[block - away, b] = summed[b * per_block : (b + 1) * per_block].astype(
                jnp.bfloat16
            )

        @pl.loop(1, n_dp)
        def _(offset):
            b = (g + offset) % n_dp
            pltpu.make_async_remote_copy(
                src_ref=returning.at[block - away, b],
                dst_ref=received.at[g, :, at],
                send_sem=part_sem,
                recv_sem=back_sem,
                device_id={"section": s, "dp": b},
                device_id_type=MESH,
            ).start()

        pltpu.make_async_copy(
            returning.at[block - away, g], received.at[g, :, at], own_sem
        ).start()

    own_row = received.at[g]
    pltpu.make_async_copy(own_row, own_row, own_sem).wait()
    rest = received.at[pl.ds(0, n_dp - 1)]
    pltpu.make_async_copy(rest, rest, back_sem).wait()

    shares = [
        jnp.broadcast_to(coefficient[:, e : e + 1], (per_block, width)) for e in range(experts)
    ]
    per_expert = n_dp // experts

    total = jnp.zeros((per_block, width), jnp.float32)
    for b in range(n_dp):
        total += shares[b // per_expert] * received[b].astype(jnp.float32)
    mixed[...] = total.astype(jnp.bfloat16)
    mixed_copy = pltpu.make_async_copy(mixed, mixed_hbm, out_sem.at[1])
    mixed_copy.start()

    pltpu.make_async_copy(others, others, send_sem).wait()
    pltpu.make_async_copy(rest, rest, part_sem).wait()
    pltpu.make_async_copy(terms, terms, term_sem.at[0]).wait()
    attended_copy.wait()
    mixed_copy.wait()


def per_device(tokens, expert_ids, router, w_up, w_down, attn_queries, attn_keys, attn_values):
    n_sec, n_dp = lax.axis_size("section"), lax.axis_size("dp")
    per_block, width = tokens.shape
    model, experts = router.shape
    ff = w_up.shape[2]
    length = attn_queries.shape[1]
    devices = n_sec * n_dp
    rows, cols = math.gcd(model, ff), math.gcd(ff, width)
    down_blocks = model // cols
    bf16, f32 = jnp.bfloat16, jnp.float32
    any_spec = pl.BlockSpec(memory_space=pl.ANY)
    return pl.pallas_call(
        functools.partial(kernel, (n_sec, n_dp, rows, cols, experts)),
        out_shape=(
            jax.ShapeDtypeStruct(tokens.shape, bf16),
            jax.ShapeDtypeStruct(attn_queries.shape, bf16),
        ),
        in_specs=[any_spec] * 8,
        out_specs=(any_spec, any_spec),
        scratch_shapes=[
            pltpu.VMEM((model * ff // cols, cols), bf16),
            pltpu.VMEM((devices, per_block, width), bf16),
            pltpu.VMEM((n_dp * per_block, model), bf16),
            pltpu.VMEM((n_dp * per_block, ff), bf16),
            pltpu.VMEM((down_blocks - width // cols, n_dp * per_block, cols), bf16),
            pltpu.VMEM((n_sec - 1, n_dp * per_block, width), bf16),
            pltpu.VMEM((width // cols, n_dp, per_block, cols), bf16),
            pltpu.VMEM((n_dp, per_block, width), bf16),
            pltpu.VMEM((experts, model), bf16),
            pltpu.VMEM((2, per_block), jnp.int32),
            pltpu.VMEM((n_dp * per_block, experts), f32),
            pltpu.VMEM((length, width), bf16),
            pltpu.VMEM((length, width), bf16),
            pltpu.VMEM((length, width), bf16),
            pltpu.VMEM((length, width), bf16),
            pltpu.VMEM((per_block, width), bf16),
            pltpu.SemaphoreType.DMA((6,)),
            pltpu.SemaphoreType.DMA((ff // cols,)),
            pltpu.SemaphoreType.DMA((down_blocks,)),
            pltpu.SemaphoreType.DMA,
            pltpu.SemaphoreType.DMA((n_dp // 2,)),
            pltpu.SemaphoreType.DMA,
            pltpu.SemaphoreType.DMA,
            pltpu.SemaphoreType.DMA((2,)),
            pltpu.SemaphoreType.DMA,
            pltpu.SemaphoreType.DMA,
            pltpu.SemaphoreType.DMA,
            pltpu.SemaphoreType.DMA((2,)),
        ],
        compiler_params=pltpu.CompilerParams(
            collective_id=0, has_side_effects=True, vmem_limit_bytes=67043328
        ),
    )(tokens, expert_ids.T, router.T, w_up, w_down, attn_queries, attn_keys, attn_values)


def solution(mesh):
    placed = (
        P("dp", "section"),
        P("dp", None),
        P(),
        P("dp", None, "section"),
        P("dp", "section", None),
        P("dp", None, "section"),
        P("dp", None, "section"),
        P("dp", None, "section"),
    )
    return jax.shard_map(
        per_device,
        mesh=mesh,
        in_specs=placed,
        out_specs=(P("dp", "section"), P("dp", None, "section")),
        check_vma=False,
    )
```
